32 devices in a mesh: row: 8 (over y, x, core), col: 4 (over z).
Axes of the slice: x: 2, y: 2, z: 4, core: 2. Of those that a mesh axis runs over, the one named last changes fastest.
Arguments:
- density: float32 [256, 256, 256], P('row', 'col'), may hold values from -5 to 5
- green_octant: float32 [256, 256, 256], P('row', 'col'), may hold values from 0 to 0.25
Outputs:
- potential: float32 [256, 256, 256], P('row', 'col')
The draws below stay inside these ranges and needn't reach their ends.
All inputs are finite; a program needn't handle non-finite values.
Results may differ from the reference program's by a relative error of at most 0.000092.
Values sent between devices are 32-bit elements; how exact they have to be, the bound alone decides.
A program may use at most 192 MiB of HBM per device.

```python
import math
import jax
import jax.numpy as jnp
from jax import lax

N = 256


def draw_density(key, part):
    noise = jax.random.normal(key, (N, N, N), jnp.float32)
    return jnp.clip(noise, -5.0, 5.0)


def draw_green_octant(key, part):
    coords = jnp.arange(N, dtype=jnp.float32)
    radius = jnp.sqrt(coords[:, None, None] * coords[:, None, None] + coords[None, :, None] * coords[None, :, None] + coords[None, None, :] * coords[None, None, :])
    factor = jnp.exp(jax.random.uniform(key, (N, N, N), jnp.float32, math.log(0.5), math.log(1.5)))
    return factor * jnp.exp(-radius / (N / 4.0)) / (4.0 * math.pi * jnp.maximum(radius, 0.5))


def setup_inputs(seed: int = 0) -> dict:
    streams_of = jax.random.split(jax.random.key(seed), 3)
    return {
        "density": draw_density(jax.random.fold_in(streams_of[2], 71), 0),
        "green_octant": draw_green_octant(jax.random.fold_in(streams_of[2], 71), 0),
    }


def cosine_table(extent, padded):
    positions = jnp.arange(extent, dtype=jnp.int32)[:, None]
    waves = jnp.arange(padded, dtype=jnp.int32)[None, :]
    phases = (positions * waves) % padded
    angles = phases.astype(jnp.float32) * jnp.float32(2.0 * 3.141592653589793 / padded)
    weights = jnp.where(positions == 0, jnp.float32(1.0), jnp.float32(2.0))
    return weights * jnp.cos(angles)


def reference(density, green_octant):
    padded = 2 * N
    table = cosine_table(N, padded)
    half_table = table[:, : N + 1]
    along_z = jnp.dot(green_octant.reshape(N * N, N), half_table, precision=lax.Precision.HIGHEST, preferred_element_type=jnp.float32).reshape(N, N, N + 1)
    along_y = jnp.einsum("ijk,jl->ilk", along_z, table, precision=lax.Precision.HIGHEST)
    kernel_hat = jnp.einsum("ijk,il->ljk", along_y, table, precision=lax.Precision.HIGHEST)
    density_hat = jnp.fft.rfftn(density, s=(padded, padded, padded))
    product = density_hat * kernel_hat
    whole = jnp.fft.irfftn(product, s=(padded, padded, padded))
    return whole[:N, :N, :N].astype(jnp.float32)
```

```python
import jax
import jax.numpy as jnp
import numpy as np
from jax import lax
from jax.experimental import pallas as pl
from jax.experimental.pallas import tpu as pltpu
from jax.sharding import PartitionSpec as P

F32 = jnp.float32
BF16 = jnp.bfloat16
VMEM_BYTES = 60 * 1024 * 1024


def trig(extent):
    k = np.arange(extent)[:, None]
    n = np.arange(extent)[None, :]
    phase = ((2 * k + 1) * n) % (4 * extent)
    angle = 2.0 * np.pi * phase / (4 * extent)
    weight = np.where(n == 0, 1.0, 2.0)
    return np.cos(angle), np.sin(angle), weight * np.cos(angle)


def halves(table):
    table = np.asarray(table, np.float32)
    high = table.astype(BF16)
    low = (table - high.astype(np.float32)).astype(BF16)
    return jnp.asarray(np.stack([high, low]))


def split(value):
    high = value.astype(BF16)
    return high, (value - high.astype(F32)).astype(BF16)


def dot3(left, right, dims=((1,), (0,))):
    def one(a, b):
        return lax.dot_general(a, b, (dims, ((), ())), preferred_element_type=F32)

    return one(left[0], right[0]) + (one(left[0], right[1]) + one(left[1], right[0]))


def forward_z_kernel(groups, dens_ref, green_ref, wave_ref, even_ref, dens_out, green_out):
    step = pl.program_id(0)
    tiles = dens_ref.shape[0] // 128
    for ref, table, out in ((dens_ref, wave_ref, dens_out), (green_ref, even_ref, green_out)):
        result = dot3((table[0], table[1]), split(ref[...]), ((1,), (1,)))
        for tile in range(tiles):
            rows = pl.ds(step * tiles + tile, result.shape[0], stride=groups)
            out[rows, :] = result[:, tile * 128 : (tile + 1) * 128]


def plane_kernel(sizes, dens_ref, green_ref, y_ref, ky_ref, x_ref, kx_ref, xi_ref, yi_ref, out_ref):
    nrow, ncol, groups, per, width = sizes
    rows = nrow * groups

    def plane(block):
        block = block.reshape(nrow, ncol, groups, 128)
        return jnp.concatenate(
            [
                jnp.concatenate(
                    [
                        block[:, c, :, h * width : (h + 1) * width].reshape(rows, width)
                        for c in range(ncol)
                    ],
                    axis=1,
                )
                for h in range(per)
            ],
            axis=0,
        )

    def pair(ref):
        return ref[0], ref[1]

    green = dot3(split(plane(green_ref[:, 0])), pair(ky_ref))
    green = dot3(pair(kx_ref), split(green))
    green = jnp.concatenate([green, green], axis=1)
    green = jnp.concatenate([green, green], axis=0)
    for part in range(2):
        value = dot3(split(plane(dens_ref[:, part, 0])), pair(y_ref))
        value = dot3(pair(x_ref), split(value)) * green
        value = dot3(pair(xi_ref), split(value))
        value = dot3(split(value), pair(yi_ref))
        blocks = [
            value[h * rows : (h + 1) * rows].reshape(nrow, groups, ncol * width)
            for h in range(per)
        ]
        for c in range(ncol):
            piece = jnp.concatenate([b[:, :, c * width : (c + 1) * width] for b in blocks], axis=2)
            for r in range(nrow):
                out_ref[r * ncol + c, part, 0] = piece[r]


def inverse_z_kernel(groups, in_ref, wave_ref, out_ref):
    step = pl.program_id(0)
    tiles = out_ref.shape[0] // 128
    count = in_ref.shape[0] // groups
    for tile in range(tiles):
        value = in_ref[pl.ds(step * tiles + tile, count, stride=groups), :]
        result = dot3((wave_ref[0], wave_ref[1]), split(value))
        out_ref[pl.ds(tile * 128, 128), :] = result.T


def whole(array):
    zeros = (0,) * len(array.shape)
    return pl.BlockSpec(array.shape, lambda i: zeros)


def make(mesh):
    nrow, ncol = mesh.shape["row"], mesh.shape["col"]
    ndev = nrow * ncol

    def on_device(density, green_octant):
        xl, width, extent = density.shape
        slots = extent // ndev
        per = 128 // width
        groups = xl // per
        cells = xl * width
        cosine, sine, even = trig(extent)
        waves = np.stack(
            [cosine.reshape(ndev, slots, extent), sine.reshape(ndev, slots, extent)], axis=1
        ).reshape(2 * extent, extent)
        both = np.concatenate([cosine, sine], axis=0)
        order = np.arange(extent).reshape(nrow, groups, per).transpose(2, 0, 1).reshape(-1)
        scale = 1.0 / extent

        params = pltpu.CompilerParams(vmem_limit_bytes=VMEM_BYTES)
        block = min(256, cells)
        z_tables = (halves(waves), halves(even))
        dens, green = pl.pallas_call(
            lambda *refs: forward_z_kernel(groups, *refs),
            grid=(cells // block,),
            in_specs=[pl.BlockSpec((block, extent), lambda i: (i, 0))] * 2
            + [whole(t) for t in z_tables],
            out_specs=[
                pl.BlockSpec((2 * extent * groups, 128), lambda i: (0, 0)),
                pl.BlockSpec((extent * groups, 128), lambda i: (0, 0)),
            ],
            out_shape=[
                jax.ShapeDtypeStruct((2 * extent * groups, 128), F32),
                jax.ShapeDtypeStruct((extent * groups, 128), F32),
            ],
            compiler_params=params,
            name="forward_z",
        )(density.reshape(cells, extent), green_octant.reshape(cells, extent), *z_tables)

        dens = dens.reshape(ndev, 2, slots, groups, 128)
        green = green.reshape(ndev, slots, groups, 128)
        axes = ("row", "col")
        green = lax.all_to_all(green, axes, split_axis=0, concat_axis=0, tiled=True)
        dens = lax.all_to_all(dens, axes, split_axis=0, concat_axis=0, tiled=True)

        tables = (
            halves(both.T),
            halves(even.T),
            halves(both[:, order]),
            halves(even[:, order]),
            halves(both[:, order].T * scale),
            halves(both * scale),
        )
        spec = pl.BlockSpec((ndev, 2, 1, groups, 128), lambda i: (0, 0, i, 0, 0))
        sizes = (nrow, ncol, groups, per, width)
        result = pl.pallas_call(
            lambda *refs: plane_kernel(sizes, *refs),
            grid=(slots,),
            in_specs=[spec, pl.BlockSpec((ndev, 1, groups, 128), lambda i: (0, i, 0, 0))]
            + [whole(t) for t in tables],
            out_specs=spec,
            out_shape=jax.ShapeDtypeStruct(dens.shape, F32),
            compiler_params=params,
            name="planes",
        )(dens, green, *tables)

        result = lax.all_to_all(result, axes, split_axis=0, concat_axis=0, tiled=True)
        back = halves(waves.T * scale)
        out = pl.pallas_call(
            lambda *refs: inverse_z_kernel(groups, *refs),
            grid=(cells // block,),
            in_specs=[
                pl.BlockSpec((2 * extent * groups, 128), lambda i: (0, 0)),
                whole(back),
            ],
            out_specs=pl.BlockSpec((block, extent), lambda i: (i, 0)),
            out_shape=jax.ShapeDtypeStruct((cells, extent), F32),
            compiler_params=params,
            name="inverse_z",
        )(result.reshape(2 * extent * groups, 128), back)
        return out.reshape(xl, width, extent)

    return on_device


def solution(mesh):
    return jax.shard_map(
        make(mesh),
        mesh=mesh,
        in_specs=(P("row", "col", None), P("row", "col", None)),
        out_specs=P("row", "col", None),
        check_vma=False,
    )
```

```python
import jax
import jax.numpy as jnp
import numpy as np
from jax import lax
from jax.experimental import pallas as pl
from jax.experimental.pallas import tpu as pltpu
from jax.sharding import PartitionSpec as P

F32 = jnp.float32
BF16 = jnp.bfloat16
VMEM_BYTES = 60 * 1024 * 1024


def trig(extent):
    k = np.arange(extent)[:, None]
    n = np.arange(extent)[None, :]
    phase = ((2 * k + 1) * n) % (4 * extent)
    angle = 2.0 * np.pi * phase / (4 * extent)
    weight = np.where(n == 0, 1.0, 2.0)
    return np.cos(angle), np.sin(angle), weight * np.cos(angle)


def halves(table):
    table = np.asarray(table, np.float32)
    high = table.astype(BF16)
    low = (table - high.astype(np.float32)).astype(BF16)
    return jnp.asarray(np.stack([high, low]))


def split(value):
    high = value.astype(BF16)
    return high, (value - high.astype(F32)).astype(BF16)


def dot3(left, right, dims=((1,), (0,))):
    def one(a, b):
        return lax.dot_general(a, b, (dims, ((), ())), preferred_element_type=F32)

    return one(left[0], right[0]) + (one(left[0], right[1]) + one(left[1], right[0]))


def fused_kernel(sizes, dens_ref, green_ref, wave_ref, even_ref, y_ref, ky_ref, x_ref, kx_ref,
                 xi_ref, yi_ref, back_ref, out_ref, dens_two, green_two, send, recv, bsend, brecv,
                 total, send_sem, recv_sem, bsend_sem, brecv_sem):
    nrow, ncol, groups, per, width, chunks, each, parts = sizes
    ndev = nrow * ncol
    rows = nrow * groups
    cells = dens_ref.shape[0]
    me = lax.axis_index("row") * ncol + lax.axis_index("col")
    size, bsize = each * 3 * groups, each * 2 * groups

    def other(step):
        target = lax.rem(me + step, ndev)
        return target, (lax.div(target, ncol), lax.rem(target, ncol))

    barrier = pltpu.get_barrier_semaphore()

    def greet(step, carry):
        pl.semaphore_signal(
            barrier, inc=1, device_id=other(step)[1], device_id_type=pl.DeviceIdType.MESH
        )
        return carry

    lax.fori_loop(1, ndev, greet, 0)

    def pair(ref):
        return ref[0], ref[1]

    def block(ref, chunk, owner, length):
        start = pl.multiple_of((chunk * ndev + owner) * length, 8)
        return ref.at[pl.ds(start, length), :]

    def spread(source, target, length, chunk, out_sem, in_sem):
        def one(step, carry):
            owner, device = other(step)
            pltpu.make_async_remote_copy(
                src_ref=block(source, chunk, owner, length),
                dst_ref=block(target, chunk, me, length),
                send_sem=out_sem.at[chunk],
                recv_sem=in_sem.at[chunk],
                device_id=device,
                device_id_type=pl.DeviceIdType.MESH,
            ).start()
            return carry

        lax.fori_loop(1, ndev, one, 0)
        block(target, chunk, me, length)[...] = block(source, chunk, me, length)[...]

    def landed(ref, length, chunk, sem):
        start = pl.multiple_of(chunk * ndev * length, 8)
        view = ref.at[pl.ds(start, (ndev - 1) * length), :]
        pltpu.make_async_copy(view, view, sem.at[chunk]).wait()

    for ref, two in ((dens_ref, dens_two), (green_ref, green_two)):
        high, low = split(ref[...])
        two[0] = high
        two[1] = low

    lines = ndev * each
    step_cells = min(256, cells)

    def transform(chunk):
        for two, table, first, count in (
            (dens_two, wave_ref, 0, 2),
            (green_two, even_ref, 2, 1),
        ):
            left = (table[0, chunk], table[1, chunk])
            for begin in range(0, cells, step_cells):
                right = (two[0, begin : begin + step_cells], two[1, begin : begin + step_cells])
                result = dot3(left, right, ((1,), (1,)))
                for part in range(count):
                    for tile in range(step_cells // 128):
                        group = begin // 128 + tile
                        start = chunk * ndev * size + (first + part) * groups + group
                        send[pl.ds(start, lines, stride=3 * groups), :] = result[
                            part * lines : (part + 1) * lines, tile * 128 : (tile + 1) * 128
                        ]

    transform(0)
    pl.semaphore_wait(barrier, ndev - 1)
    spread(send, recv, size, 0, send_sem, recv_sem)

    def forward(chunk, carry):
        transform(chunk)
        spread(send, recv, size, chunk, send_sem, recv_sem)
        return carry

    lax.fori_loop(1, chunks, forward, 0)

    def planes(chunk, carry):
        landed(recv, size, chunk, recv_sem)

        def load(slot, part):
            def piece(r, c):
                start = ((chunk * ndev + r * ncol + c) * each + slot) * 3 * groups + part * groups
                return recv[pl.ds(start, groups), :]

            columns = [
                jnp.concatenate([piece(r, c) for r in range(nrow)], axis=0) for c in range(ncol)
            ]
            return jnp.concatenate(
                [
                    jnp.concatenate([v[:, h * width : (h + 1) * width] for v in columns], axis=1)
                    for h in range(per)
                ],
                axis=0,
            )

        def one_slot(slot, inner):
            green = dot3(split(load(slot, 2)), pair(ky_ref))
            green = dot3(pair(kx_ref), split(green))
            green = jnp.concatenate([green, green], axis=1)
            green = jnp.concatenate([green, green], axis=0)
            for part in range(2):
                value = dot3(split(load(slot, part)), pair(y_ref))
                value = dot3(pair(x_ref), split(value)) * green
                value = dot3(pair(xi_ref), split(value))
                value = dot3(split(value), pair(yi_ref))
                for c in range(ncol):
                    piece = jnp.concatenate(
                        [
                            value[h * rows : (h + 1) * rows, c * width : (c + 1) * width]
                            for h in range(per)
                        ],
                        axis=1,
                    )
                    for r in range(nrow):
                        start = ((chunk * ndev + r * ncol + c) * each + slot) * 2 * groups
                        start = start + part * groups
                        bsend[pl.ds(start, groups), :] = piece[r * groups : (r + 1) * groups]
            return inner

        lax.fori_loop(0, each, one_slot, 0)
        spread(bsend, brecv, bsize, chunk, bsend_sem, brecv_sem)
        return carry

    lax.fori_loop(0, chunks, planes, 0)

    depth = 2 * lines * chunks // parts
    for half in range(parts):
        for chunk in range(half * chunks // parts, (half + 1) * chunks // parts):
            landed(brecv, bsize, chunk, brecv_sem)
        for group in range(groups):
            value = brecv[pl.ds(half * depth * groups + group, depth, stride=groups), :]
            table = (back_ref[0, half], back_ref[1, half])
            result = dot3(table, split(value))
            if half > 0:
                result = result + total[:, group * 128 : (group + 1) * 128]
            if half < parts - 1:
                total[:, group * 128 : (group + 1) * 128] = result
            else:
                out_ref[pl.ds(group * 128, 128), :] = result.T

    def finish(chunk, carry):
        landed(send, size, chunk, send_sem)
        landed(bsend, bsize, chunk, bsend_sem)
        return carry

    lax.fori_loop(0, chunks, finish, 0)


def make(mesh):
    nrow, ncol = mesh.shape["row"], mesh.shape["col"]
    ndev = nrow * ncol

    def on_device(density, green_octant):
        xl, width, extent = density.shape
        slots = extent // ndev
        per = 128 // width
        groups = xl // per
        cells = xl * width
        each = min(2, slots)
        chunks = slots // each
        parts = 2 if chunks % 2 == 0 else 1
        cosine, sine, even = trig(extent)

        def chunked(table):
            return table.reshape(ndev, chunks, each, extent).transpose(1, 0, 2, 3)

        lines = ndev * each
        waves = np.stack([chunked(cosine), chunked(sine)], axis=1).reshape(
            chunks, 2 * lines, extent
        )
        evens = chunked(even).reshape(chunks, lines, extent)
        back = np.stack([chunked(cosine), chunked(sine)], axis=3).reshape(parts, -1, extent)
        back = back.transpose(0, 2, 1)
        both = np.concatenate([cosine, sine], axis=0)
        order = np.arange(extent).reshape(nrow, groups, per).transpose(2, 0, 1).reshape(-1)
        scale = 1.0 / extent
        tables = (
            halves(waves),
            halves(evens),
            halves(both.T),
            halves(even.T),
            halves(both[:, order]),
            halves(even[:, order]),
            halves(both[:, order].T * scale),
            halves(both * scale),
            halves(back * scale),
        )
        operands = (
            density.reshape(cells, extent),
            green_octant.reshape(cells, extent),
        ) + tables
        size, bsize = each * 3 * groups, each * 2 * groups
        sizes = (nrow, ncol, groups, per, width, chunks, each, parts)
        out = pl.pallas_call(
            lambda *refs: fused_kernel(sizes, *refs),
            in_specs=[pl.BlockSpec(memory_space=pltpu.VMEM)] * len(operands),
            out_specs=pl.BlockSpec(memory_space=pltpu.VMEM),
            out_shape=jax.ShapeDtypeStruct((cells, extent), F32),
            scratch_shapes=[
                pltpu.VMEM((2, cells, extent), BF16),
                pltpu.VMEM((2, cells, extent), BF16),
                pltpu.VMEM((chunks * ndev * size, 128), F32),
                pltpu.VMEM((chunks * ndev * size, 128), F32),
                pltpu.VMEM((chunks * ndev * bsize, 128), F32),
                pltpu.VMEM((chunks * ndev * bsize, 128), F32),
                pltpu.VMEM((extent, cells), F32),
            ]
            + [pltpu.SemaphoreType.DMA((chunks,))] * 4,
            compiler_params=pltpu.CompilerParams(
                vmem_limit_bytes=VMEM_BYTES, collective_id=0, has_side_effects=True
            ),
            name="fused",
        )(*operands)
        return out.reshape(xl, width, extent)

    return on_device


def solution(mesh):
    return jax.shard_map(
        make(mesh),
        mesh=mesh,
        in_specs=(P("row", "col", None), P("row", "col", None)),
        out_specs=P("row", "col", None),
        check_vma=False,
    )
```
